128 devices in a mesh: row: 16 (over x_hi, y, core), col: 8 (over x_lo, z).
Axes of the slice: x: 4 (x_hi: 2, x_lo: 2; x = x_hi * 2 + x_lo), y: 4, z: 4, core: 2. Of those that a mesh axis runs over, the one named last changes fastest.
Arguments:
- object_core: float32 [4, 4096, 2048], P(None, 'row', 'col'), may hold values from -4.2 to 4.2
- probe_field: float32 [2, 256, 256], replicated, may hold values from -4.2 to 4.2
- offsets: int32 [16, 8, 3, 2], P('row', 'col'), may hold values from 0 to 256
- tile_counts: int32 [16, 8], P('row', 'col'), may hold values from 1 to 3, as said below
- intensity: float32 [16, 8, 3, 256, 256], P('row', 'col'), may hold values from 0.25 to 2
Outputs:
- object_next: float32 [4, 4096, 2048], P(None, 'row', 'col')
The draws below stay inside these ranges and needn't reach their ends.
Inputs may be any that keep to these rules, and one draw needn't show every extreme that they name: offsets of the probe window inside a tile's patch of side 512; slots at or past the tile's count are unused. `tile_counts`: some tile holds 3 positions.
All inputs are finite; a program needn't handle non-finite values.
Results may differ from the reference program's by a relative error of at most 0.0003.
Values sent between devices are 32-bit elements; how exact they have to be, the bound alone decides.
No kernel may reach another device: no remote copies, remote signals or barrier semaphores. Data moves between devices by JAX's collectives and lax.ppermute only.
A program may use at most 128 MiB of HBM per device.

```python
import jax
import jax.numpy as jnp
from jax import lax

PROBE = 256
CORE = 256
MARGIN = 128
PATCH = 512
SLICES = 2
SLOTS = 3
ITERS = 2
OBJ_ROWS = 4096
OBJ_COLS = 2048
N_ROW = 16
N_COL = 8


def draw_tile_counts(key, part):
    counted = jax.random.randint(key, (N_ROW * N_COL,), 1, SLOTS + 1, dtype=jnp.int32)
    chosen = jax.random.randint(jax.random.fold_in(key, 7), (), 0, N_ROW * N_COL, dtype=jnp.int32)
    counted = counted.at[chosen].set(SLOTS)
    return counted.reshape(N_ROW, N_COL)


def with_ends(values, stream_key, smallest, largest):
    longest = values.shape.index(max(values.shape))
    spots = []
    for shift in (0, 1):
        where = [jax.random.randint(jax.random.fold_in(stream_key, axis), (), 0, length) for axis, length in enumerate(values.shape)]
        where[longest] = (where[longest] + shift) % values.shape[longest]
        spots.append(tuple(where))
    return values.at[spots[0]].set(smallest).at[spots[1]].set(largest)


def block_levels(key, dims, cuts, least, largest):
    def one(dim, parts):
        heights = jax.random.uniform(jax.random.fold_in(jax.random.fold_in(key, 6), dim), (parts,), jnp.float32, least / len(cuts), largest / len(cuts))
        return jnp.repeat(jnp.exp(heights), dims[dim] // parts).reshape((-1,) + (1,) * (len(dims) - dim - 1))

    level = one(*cuts[0])
    for cut in cuts[1:]:
        level = level * one(*cut)
    return level


def noise(own_key, dims, width, limit, cuts=(), held_as=jnp.bfloat16):
    factor_of = block_levels(own_key, dims, cuts, -0.22, 0.18) if cuts else 1.0
    result = jax.random.normal(own_key, dims, jnp.float32) * width * factor_of
    return jnp.minimum(jnp.maximum(result, -limit), limit).astype(held_as)


def setup_inputs(seed: int = 0) -> dict:
    splits = jax.random.split(jax.random.key(seed), 6)
    object_core = noise(splits[0], (2 * SLICES, OBJ_ROWS, OBJ_COLS), 0.7, 4.2, ((1, 16), (2, 8)), jnp.float32)
    probe_field = noise(splits[1], (2, PROBE, PROBE), 0.7, 4.2, (), jnp.float32)
    offsets = with_ends(jax.random.randint(splits[2], (N_ROW, N_COL, SLOTS, 2), 0, PATCH - PROBE + 1), jax.random.fold_in(splits[2], 1), 0, PATCH - PROBE).astype(jnp.int32)
    tile_counts = draw_tile_counts(jax.random.fold_in(splits[5], 71), 0)
    intensity = jnp.clip(0.25 + 1.75 * jax.random.uniform(splits[4], (N_ROW, N_COL, SLOTS, PROBE, PROBE), jnp.float32) ** block_levels(splits[4], (N_ROW, N_COL, SLOTS, PROBE, PROBE), ((0, 16), (1, 8)), -0.2, 0.2), 0.25, 2.0)
    return dict(object_core=object_core, probe_field=probe_field, offsets=offsets, tile_counts=tile_counts, intensity=intensity)


FRESNEL = 24.0
STEP_SIZE = 0.05


def propagator():
    shifted = (jnp.arange(PROBE, dtype=jnp.int32) + PROBE // 2) % PROBE - PROBE // 2
    frequency = shifted.astype(jnp.float32) / PROBE
    phase = -jnp.pi * FRESNEL * (frequency[:, None] ** 2 + frequency[None, :] ** 2)
    return jnp.cos(phase) + 1j * jnp.sin(phase)


def forward_fft(field):
    return jnp.fft.fft2(field, norm="ortho")


def inverse_fft(field):
    return jnp.fft.ifft2(field, norm="ortho")


def position_gradient(window, incident, measured, kernel, weight):
    layers = [window[2 * number] + 1j * window[2 * number + 1] for number in range(SLICES)]
    current = incident
    entering = []
    for number in range(SLICES):
        if number > 0:
            current = inverse_fft(kernel * forward_fft(current))
        entering.append(current)
        current = current * layers[number]
    farfield = forward_fft(current)
    squared = jnp.real(farfield) ** 2 + jnp.imag(farfield) ** 2
    backward = inverse_fft(weight * (squared - measured) * farfield)
    pieces = [None] * SLICES
    for number in reversed(range(SLICES)):
        if number < SLICES - 1:
            backward = inverse_fft(jnp.conj(kernel) * forward_fft(backward))
        contrib = jnp.conj(entering[number]) * backward
        pieces[number] = jnp.stack([jnp.real(contrib), jnp.imag(contrib)])
        backward = jnp.conj(layers[number]) * backward
    return jnp.concatenate(pieces, axis=0)


def fold_axis(extended, axis_number):
    length = extended.shape[axis_number]
    inner = lax.slice_in_dim(extended, MARGIN, length - MARGIN, axis=axis_number)
    inner_length = length - 2 * MARGIN
    head = lax.slice_in_dim(inner, 0, MARGIN, axis=axis_number) + lax.slice_in_dim(extended, length - MARGIN, length, axis=axis_number)
    middle = lax.slice_in_dim(inner, MARGIN, inner_length - MARGIN, axis=axis_number)
    tail = lax.slice_in_dim(inner, inner_length - MARGIN, inner_length, axis=axis_number) + lax.slice_in_dim(extended, 0, MARGIN, axis=axis_number)
    return jnp.concatenate([head, middle, tail], axis=axis_number)


def reference(object_core, probe_field, offsets, tile_counts, intensity):
    kernel = propagator()
    incident = probe_field[0] + 1j * probe_field[1]
    current = object_core
    for iteration in range(ITERS):
        extended = jnp.pad(current, ((0, 0), (MARGIN, MARGIN), (MARGIN, MARGIN)), mode="wrap")

        def visit(gathered, tile_id):
            tile_row = tile_id // N_COL
            tile_col = tile_id % N_COL
            for number in range(SLOTS):
                start_row = (tile_row * CORE + offsets[tile_row, tile_col, number, 0]).astype(jnp.int32)
                start_col = (tile_col * CORE + offsets[tile_row, tile_col, number, 1]).astype(jnp.int32)
                anchor = (jnp.int32(0), start_row, start_col)
                window = lax.dynamic_slice(extended, anchor, (2 * SLICES, PROBE, PROBE))
                weight = (number < tile_counts[tile_row, tile_col]).astype(jnp.float32)
                contrib = position_gradient(window, incident, intensity[tile_row, tile_col, number], kernel, weight)
                updated = lax.dynamic_slice(gathered, anchor, (2 * SLICES, PROBE, PROBE)) + contrib.astype(gathered.dtype)
                gathered = lax.dynamic_update_slice(gathered, updated, anchor)
            return gathered, None

        gathered, unused = lax.scan(visit, jnp.zeros(extended.shape, jnp.float32), jnp.arange(N_ROW * N_COL, dtype=jnp.int32))
        summed = fold_axis(fold_axis(gathered, 1), 2)
        current = current - STEP_SIZE * summed
    return current
```

```python
import functools

import jax
import jax.numpy as jnp
import numpy as np
from jax import lax
from jax.experimental import pallas as pl
from jax.experimental.pallas import tpu as pltpu
from jax.sharding import PartitionSpec as P

PROBE = 256
HALF = 128
SLICES = 2
SLOTS = 3
ITERS = 2
CHANNELS = 2 * SLICES
FRESNEL = 24.0
STEP_SIZE = 0.05
CHUNK = 32

F32 = jnp.float32
BF16 = jnp.bfloat16
VMEM = pl.BlockSpec(memory_space=pltpu.VMEM)
SMEM = pl.BlockSpec(memory_space=pltpu.SMEM)

FE, FO, PU, PV, FET, FOT, PUT, PVT = range(8)


def real_form(matrix):
    return np.block([[matrix.real, matrix.imag], [-matrix.imag, matrix.real]])


def tables():
    n = np.arange(HALF)
    even = np.exp(-2j * np.pi * ((2 * np.outer(n, n)) % PROBE) / PROBE) / math_root()
    odd = np.exp(-2j * np.pi * ((n[:, None] * (2 * n[None, :] + 1)) % PROBE) / PROBE) / math_root()
    whole = np.arange(PROBE)
    frequency = ((whole + HALF) % PROBE - HALF) / PROBE
    response = np.exp(-1j * np.pi * FRESNEL * frequency**2)
    first = np.fft.ifft(response)
    circulant = first[(whole[:, None] - whole[None, :]) % PROBE]
    near, far = circulant[:HALF, :HALF], circulant[:HALF, HALF:]
    forms = [real_form(m) for m in (even, odd, (near + far) / 2, (near - far) / 2)]
    forms = np.stack(forms + [m.T for m in forms]).astype(np.float32)
    high = forms.astype(BF16)
    low = (forms - high.astype(np.float32)).astype(BF16)
    return np.concatenate([high, low])


def math_root():
    return float(np.sqrt(PROBE))


def order_table():
    order = np.concatenate([np.arange(0, PROBE, 2), np.arange(1, PROBE, 2)])
    table = np.zeros((PROBE, PROBE), np.float32)
    table[order, np.arange(PROBE)] = 1.0
    return np.stack([table, table.T]).astype(BF16)


def dot(left, right):
    return jnp.dot(left, right, preferred_element_type=F32)


def parts(values):
    high = values.astype(BF16)
    low = (values - high.astype(F32)).astype(BF16)
    return high, low


def right_dot(values, tab, number):
    high, low = parts(values)
    return dot(high, tab[number]) + (dot(low, tab[number]) + dot(high, tab[number + 8]))


def left_dot(tab, number, values):
    high, low = parts(values)
    return dot(tab[number], high) + (dot(tab[number + 8], high) + dot(tab[number], low))


def halves(values, axis):
    if axis == 1:
        return values[:, :HALF], values[:, HALF:]
    return values[:HALF, :], values[HALF:, :]


def pass_along(real, imag, axis, tab, first, second, before, after):
    r0, r1 = halves(real, axis)
    i0, i1 = halves(imag, axis)
    if before:
        r0, r1, i0, i1 = r0 + r1, r0 - r1, i0 + i1, i0 - i1
    u = jnp.concatenate([r0, i0], axis=axis)
    v = jnp.concatenate([r1, i1], axis=axis)
    if axis == 1:
        u, v = right_dot(u, tab, first), right_dot(v, tab, second)
    else:
        u, v = left_dot(tab, first, u), left_dot(tab, second, v)
    r0, i0 = halves(u, axis)
    r1, i1 = halves(v, axis)
    if after:
        r0, r1, i0, i1 = r0 + r1, r0 - r1, i0 + i1, i0 - i1
    return jnp.concatenate([r0, r1], axis=axis), jnp.concatenate([i0, i1], axis=axis)


def outside(shape, axis, base, offset):
    place = lax.broadcasted_iota(jnp.int32, shape, axis) + base
    start = offset - HALF
    return (place < start) | (place >= start + PROBE)


def prepare_kernel(offs, probe, intensity, order, rolled, ordered, work):
    for slot in range(SLOTS):
        for part in range(2):
            value = pltpu.roll(probe[part], (offs[2 * slot] + HALF) & (PROBE - 1), 0)
            rolled[slot, part] = pltpu.roll(value, (offs[2 * slot + 1] + HALF) & (PROBE - 1), 1)
    for slot in range(SLOTS):
        value = intensity[slot]
        for axis in (1, 0):
            high = value.astype(BF16)
            rest = value - high.astype(F32)
            middle = rest.astype(BF16)
            low = (rest - middle.astype(F32)).astype(BF16)
            if axis == 1:
                value = (dot(high, order[0]) + dot(middle, order[0])) + dot(low, order[0])
                work[...] = value
                value = work[...]
            else:
                value = (dot(order[1], high) + dot(order[1], middle)) + dot(order[1], low)
        ordered[slot] = value


def gather_windows(offs, wide, row_a, row_b, slice_number, target):
    parity = offs[2 * SLOTS + 1]
    for source, half in ((row_a, parity), (row_b, 1 - parity)):

        @pl.loop(0, HALF // CHUNK)
        def _(step):
            start = pl.multiple_of(step * CHUNK, CHUNK)
            base = pl.multiple_of(half * HALF + start, CHUNK)
            for slot in range(SLOTS):
                shape = (CHUNK, PROBE)
                row_out = outside(shape, 0, base, offs[2 * slot])
                col_out = outside(shape, 1, 0, offs[2 * slot + 1])
                for part in range(2):
                    channel = 2 * slice_number + part
                    own = wide[channel, pl.ds(base, CHUNK), :]
                    other = source[channel, pl.ds(start, CHUNK), :]
                    near = jnp.where(row_out, other[:, :PROBE], own[:, :PROBE])
                    across = jnp.where(row_out, other[:, PROBE:], own[:, PROBE:])
                    target[slot, part, pl.ds(base, CHUNK), :] = jnp.where(col_out, across, near)


def spread(offs, contrib, slice_number, kept, send_a, send_b):
    parity = offs[2 * SLOTS + 1]
    for target, half in ((send_a, parity), (send_b, 1 - parity)):

        @pl.loop(0, HALF // CHUNK)
        def _(step):
            start = pl.multiple_of(step * CHUNK, CHUNK)
            base = pl.multiple_of(half * HALF + start, CHUNK)
            shape = (CHUNK, PROBE)
            masks = [
                (outside(shape, 0, base, offs[2 * s]), outside(shape, 1, 0, offs[2 * s + 1]))
                for s in range(SLOTS)
            ]
            for part in range(2):
                channel = 2 * slice_number + part
                totals = [None] * 4
                for slot, (row_out, col_out) in enumerate(masks):
                    value = contrib[slot, part, pl.ds(base, CHUNK), :]
                    zero = jnp.zeros_like(value)
                    inner = jnp.where(row_out, zero, value)
                    outer = jnp.where(row_out, value, zero)
                    pieces = [
                        jnp.where(col_out, zero, inner),
                        jnp.where(col_out, inner, zero),
                        jnp.where(col_out, zero, outer),
                        jnp.where(col_out, outer, zero),
                    ]
                    totals = [p if t is None else t + p for t, p in zip(totals, pieces)]
                kept[channel, pl.ds(base, CHUNK), :PROBE] = totals[0]
                kept[channel, pl.ds(base, CHUNK), PROBE:] = totals[1]
                target[channel, pl.ds(start, CHUNK), :PROBE] = totals[2]
                target[channel, pl.ds(start, CHUNK), PROBE:] = totals[3]


def gradient_kernel(
    offs, wide, row_a, row_b, rolled, ordered, tab, kept, send_a, send_b, win0, win1, wave, work, held
):
    gather_windows(offs, wide, row_a, row_b, 0, win0)
    gather_windows(offs, wide, row_a, row_b, 1, win1)
    for s in range(SLOTS):
        pr, pi, wr, wi = rolled[s, 0], rolled[s, 1], win0[s, 0], win0[s, 1]
        out = pass_along(pr * wr - pi * wi, pr * wi + pi * wr, 1, tab, PU, PV, True, True)
        work[s, 0], work[s, 1] = out
    for s in range(SLOTS):
        wave[s, 0], wave[s, 1] = pass_along(
            work[s, 0], work[s, 1], 0, tab, PUT, PVT, True, True
        )
    for s in range(SLOTS):
        pr, pi, wr, wi = wave[s, 0], wave[s, 1], win1[s, 0], win1[s, 1]
        out = pass_along(pr * wr - pi * wi, pr * wi + pi * wr, 1, tab, FE, FO, True, False)
        held[s, 0], held[s, 1] = out
    for s in range(SLOTS):
        weight = jnp.where(s < offs[2 * SLOTS], 1.0, 0.0).astype(F32)
        fr, fi = pass_along(held[s, 0], held[s, 1], 0, tab, FET, FOT, True, False)
        factor = weight * (fr * fr + fi * fi - ordered[s])
        work[s, 0], work[s, 1] = factor * fr, factor * fi
    for s in range(SLOTS):
        held[s, 0], held[s, 1] = pass_along(work[s, 0], work[s, 1], 0, tab, FE, FO, False, True)
    for s in range(SLOTS):
        br, bi = pass_along(held[s, 0], held[s, 1], 1, tab, FET, FOT, False, True)
        er, ei, wr, wi = wave[s, 0], wave[s, 1], win1[s, 0], win1[s, 1]
        wave[s, 0], wave[s, 1] = er * br + ei * bi, er * bi - ei * br
        work[s, 0], work[s, 1] = wr * br + wi * bi, wr * bi - wi * br
    spread(offs, wave, 1, kept, send_a, send_b)
    for s in range(SLOTS):
        held[s, 0], held[s, 1] = pass_along(work[s, 0], work[s, 1], 1, tab, PUT, PVT, True, True)
    for s in range(SLOTS):
        br, bi = pass_along(held[s, 0], held[s, 1], 0, tab, PU, PV, True, True)
        pr, pi = rolled[s, 0], rolled[s, 1]
        work[s, 0], work[s, 1] = pr * br + pi * bi, pr * bi - pi * br
    spread(offs, work, 0, kept, send_a, send_b)


def copy_rows(parity, wide, send_a, send_b, write=None):
    for target, half in ((send_a, 1 - parity), (send_b, parity)):

        @pl.loop(0, HALF // CHUNK)
        def _(step):
            start = pl.multiple_of(step * CHUNK, CHUNK)
            base = pl.multiple_of(half * HALF + start, CHUNK)
            for channel in range(CHANNELS):
                target[channel, pl.ds(start, CHUNK), :] = write(channel, base)


def widen_kernel(offs, own, right, left, wide, send_a, send_b):
    def write(channel, base):
        rows = pl.ds(base, CHUNK)
        value = jnp.concatenate(
            [own[channel, rows, :], right[channel, rows, :], left[channel, rows, :]], axis=1
        )
        wide[channel, rows, :] = value
        return value

    copy_rows(offs[2 * SLOTS + 1], wide, send_a, send_b, write)


def fold_rows(offs, kept, row_a, row_b, write):
    parity = offs[2 * SLOTS + 1]
    for source, half in ((row_a, 1 - parity), (row_b, parity)):

        @pl.loop(0, HALF // CHUNK)
        def _(step):
            start = pl.multiple_of(step * CHUNK, CHUNK)
            base = pl.multiple_of(half * HALF + start, CHUNK)
            for channel in range(CHANNELS):
                value = kept[channel, pl.ds(base, CHUNK), :] + source[channel, pl.ds(start, CHUNK), :]
                write(channel, pl.ds(base, CHUNK), value)


def fold_middle_kernel(offs, kept, row_a, row_b, total, to_right, to_left):
    def write(channel, rows, value):
        total[channel, rows, :] = value
        to_right[channel, rows, :HALF] = value[:, 256:384]
        to_right[channel, rows, HALF:] = value[:, 128:256]
        to_left[channel, rows, :HALF] = value[:, 0:128]
        to_left[channel, rows, HALF:] = value[:, 384:512]

    fold_rows(offs, kept, row_a, row_b, write)


def fold_last_kernel(offs, kept, row_a, row_b, total, to_right, to_left):
    def write(channel, rows, value):
        total[channel, rows, :] = value[:, :256]
        to_right[channel, rows, :] = value[:, 256:384]
        to_left[channel, rows, :] = value[:, 384:512]

    fold_rows(offs, kept, row_a, row_b, write)


def update_middle_kernel(offs, wide, total, from_left, from_right, after, send_a, send_b):
    def write(channel, base):
        rows = pl.ds(base, CHUNK)
        low, high = from_left[channel, rows, :], from_right[channel, rows, :]
        came = jnp.concatenate(
            [low[:, :HALF], high[:, HALF:], high[:, :HALF], low[:, HALF:]], axis=1
        )
        value = wide[channel, rows, :] - STEP_SIZE * (total[channel, rows, :] + came)
        after[channel, rows, :] = value
        return value

    copy_rows(offs[2 * SLOTS + 1], wide, send_a, send_b, write)


def update_last_kernel(wide, total, from_left, from_right, after):
    @pl.loop(0, PROBE // CHUNK)
    def _(step):
        rows = pl.ds(pl.multiple_of(step * CHUNK, CHUNK), CHUNK)
        for channel in range(CHANNELS):
            came = jnp.concatenate(
                [from_left[channel, rows, :], from_right[channel, rows, :]], axis=1
            )
            after[channel, rows, :] = wide[channel, rows, :PROBE] - STEP_SIZE * (
                total[channel, rows, :] + came
            )


def kernel_call(body, outs, ins, scratch=(), flops=0):
    return pl.pallas_call(
        body,
        out_shape=[jax.ShapeDtypeStruct(shape, F32) for shape in outs],
        in_specs=[SMEM if kind == "s" else VMEM for kind in ins],
        out_specs=[VMEM] * len(outs),
        scratch_shapes=[pltpu.VMEM(shape, F32) for shape in scratch],
        compiler_params=pltpu.CompilerParams(vmem_limit_bytes=56 * 1024 * 1024),
        cost_estimate=pl.CostEstimate(
            flops=flops, bytes_accessed=4 * sum(int(np.prod(s)) for s in outs), transcendentals=0
        ),
    )


WIDE = (CHANNELS, PROBE, 2 * PROBE)
BAND = (CHANNELS, HALF, 2 * PROBE)
STRIP = (CHANNELS, PROBE, HALF)
CORE = (CHANNELS, PROBE, PROBE)
FIELD = (SLOTS, 2, PROBE, PROBE)


def shifted(value, axis, steps):
    count = lax.axis_size(axis)
    return lax.ppermute(value, axis, [(i, (i + steps) % count) for i in range(count)])


def swapped(value, axis, odd):
    count = lax.axis_size(axis)
    pairs = []
    for low in range(odd, count + odd, 2):
        one, two = low % count, (low + 1) % count
        pairs += [(one, two), (two, one)]
    return lax.ppermute(value, axis, pairs)


def local(object_core, probe_field, offsets, tile_counts, intensity):
    parity = lax.axis_index("row") % 2
    scalars = jnp.concatenate(
        [offsets.reshape(-1), tile_counts.reshape(-1), parity.astype(jnp.int32).reshape(1)]
    )
    tab = jnp.asarray(tables())
    order = jnp.asarray(order_table())

    right = shifted(object_core[:, :, :HALF], "col", -1)
    left = shifted(object_core[:, :, HALF:], "col", 1)
    rolled, ordered = kernel_call(
        prepare_kernel, [FIELD, (SLOTS, PROBE, PROBE)], "svvv", [(PROBE, PROBE)], 10**9
    )(scalars, probe_field, intensity[0, 0], order)
    wide, send_a, send_b = kernel_call(widen_kernel, [WIDE, BAND, BAND], "svvv", flops=10**7)(
        scalars, object_core, right, left
    )
    for iteration in range(ITERS):
        row_b = swapped(send_b, "row", 1)
        row_a = swapped(send_a, "row", 0)
        kept, send_a, send_b = kernel_call(
            gradient_kernel,
            [WIDE, BAND, BAND],
            "svvvvvv",
            [FIELD] * 5,
            10**10,
        )(scalars, wide, row_a, row_b, rolled, ordered, tab)
        row_b = swapped(send_b, "row", 1)
        row_a = swapped(send_a, "row", 0)
        last = iteration == ITERS - 1
        if last:
            total, to_right, to_left = kernel_call(
                fold_last_kernel, [CORE, STRIP, STRIP], "svvv", flops=10**7
            )(scalars, kept, row_a, row_b)
        else:
            total, to_right, to_left = kernel_call(
                fold_middle_kernel, [WIDE, CORE, CORE], "svvv", flops=10**7
            )(scalars, kept, row_a, row_b)
        from_left = shifted(to_right, "col", 1)
        from_right = shifted(to_left, "col", -1)
        if last:
            (after,) = kernel_call(update_last_kernel, [CORE], "vvvv", flops=10**7)(
                wide, total, from_left, from_right
            )
            return after
        wide, send_a, send_b = kernel_call(
            update_middle_kernel, [WIDE, BAND, BAND], "svvvv", flops=10**7
        )(scalars, wide, total, from_left, from_right)


def solution(mesh):
    placed = (
        P(None, "row", "col"),
        P(),
        P("row", "col", None, None),
        P("row", "col"),
        P("row", "col", None, None, None),
    )
    return jax.shard_map(
        local, mesh=mesh, in_specs=placed, out_specs=P(None, "row", "col"), check_vma=False
    )
```

```python
import functools

import jax
import jax.numpy as jnp
import numpy as np
from jax import lax
from jax.experimental import pallas as pl
from jax.experimental.pallas import tpu as pltpu
from jax.sharding import PartitionSpec as P

PROBE = 256
HALF = 128
SLICES = 2
SLOTS = 3
ITERS = 2
CHANNELS = 2 * SLICES
FRESNEL = 24.0
STEP_SIZE = 0.05
CHUNK = 32

F32 = jnp.float32
BF16 = jnp.bfloat16
VMEM = pl.BlockSpec(memory_space=pltpu.VMEM)
SMEM = pl.BlockSpec(memory_space=pltpu.SMEM)

E, O, ET, OT = range(4)


def real_form(matrix):
    return np.block([[matrix.real, matrix.imag], [-matrix.imag, matrix.real]])


def stack_of(one, two):
    forms = [real_form(one), real_form(two)]
    forms = np.stack(forms + [m.T for m in forms]).astype(np.float32)
    high = forms.astype(BF16)
    low = (forms - high.astype(np.float32)).astype(BF16)
    return np.concatenate([high, low])


def tables():
    n = np.arange(HALF)
    even = np.exp(-2j * np.pi * ((2 * np.outer(n, n)) % PROBE) / PROBE) / math_root()
    odd = np.exp(-2j * np.pi * ((n[:, None] * (2 * n[None, :] + 1)) % PROBE) / PROBE) / math_root()
    whole = np.arange(PROBE)
    frequency = ((whole + HALF) % PROBE - HALF) / PROBE
    response = np.exp(-1j * np.pi * FRESNEL * frequency**2)
    first = np.fft.ifft(response)
    circulant = first[(whole[:, None] - whole[None, :]) % PROBE]
    near, far = circulant[:HALF, :HALF], circulant[:HALF, HALF:]
    return stack_of(even, odd), stack_of((near + far) / 2, (near - far) / 2)


def math_root():
    return float(np.sqrt(PROBE))


def dot(left, right):
    return jnp.dot(left, right, preferred_element_type=F32)


def parts(values):
    high = values.astype(BF16)
    low = (values - high.astype(F32)).astype(BF16)
    return high, low


def right_dot(values, tab, number):
    high, low = parts(values)
    return dot(high, tab[number]) + (dot(low, tab[number]) + dot(high, tab[number + 4]))


def left_dot(tab, number, values):
    high, low = parts(values)
    return dot(tab[number], high) + (dot(tab[number + 4], high) + dot(tab[number], low))


def halves(values, axis):
    if axis == 1:
        return values[:, :HALF], values[:, HALF:]
    return values[:HALF, :], values[HALF:, :]


def pass_along(real, imag, axis, tab, first, second, before, after):
    r0, r1 = halves(real, axis)
    i0, i1 = halves(imag, axis)
    if before:
        r0, r1, i0, i1 = r0 + r1, r0 - r1, i0 + i1, i0 - i1
    u = jnp.concatenate([r0, i0], axis=axis)
    v = jnp.concatenate([r1, i1], axis=axis)
    if axis == 1:
        u, v = right_dot(u, tab, first), right_dot(v, tab, second)
    else:
        u, v = left_dot(tab, first, u), left_dot(tab, second, v)
    r0, i0 = halves(u, axis)
    r1, i1 = halves(v, axis)
    if after:
        r0, r1, i0, i1 = r0 + r1, r0 - r1, i0 + i1, i0 - i1
    return jnp.concatenate([r0, r1], axis=axis), jnp.concatenate([i0, i1], axis=axis)


def outside(shape, axis, base, offset):
    place = lax.broadcasted_iota(jnp.int32, shape, axis) + base
    start = offset - HALF
    return (place < start) | (place >= start + PROBE)


def ordering():
    row = lax.broadcasted_iota(jnp.int32, (PROBE, PROBE), 0)
    column = lax.broadcasted_iota(jnp.int32, (PROBE, PROBE), 1)
    wanted = jnp.where(column < HALF, 2 * column, 2 * column - (PROBE - 1))
    back = jnp.where(row < HALF, 2 * row, 2 * row - (PROBE - 1))
    one = jnp.where(row == wanted, 1.0, 0.0).astype(BF16)
    two = jnp.where(column == back, 1.0, 0.0).astype(BF16)
    return one, two


def prepare_kernel(offs, probe, intensity, rolled, ordered, order):
    order[0], order[1] = ordering()
    for slot in range(SLOTS):
        for part in range(2):
            value = pltpu.roll(probe[part], (offs[2 * slot] + HALF) & (PROBE - 1), 0)
            rolled[slot, part] = pltpu.roll(value, (offs[2 * slot + 1] + HALF) & (PROBE - 1), 1)

    @pl.loop(0, SLOTS)
    def _(slot):
        for axis in (1, 0):
            value = ordered[slot] if axis == 0 else intensity[slot]
            high = value.astype(BF16)
            rest = value - high.astype(F32)
            middle = rest.astype(BF16)
            low = (rest - middle.astype(F32)).astype(BF16)
            if axis == 1:
                value = (dot(high, order[0]) + dot(middle, order[0])) + dot(low, order[0])
            else:
                value = (dot(order[1], high) + dot(order[1], middle)) + dot(order[1], low)
            ordered[slot] = value


def row_halves(offs, one, two, first):
    parity = offs[2 * SLOTS + 1]
    return ((one, parity), (two, 1 - parity)) if first else ((one, 1 - parity), (two, parity))


def chunks(half):
    def run(body):
        @pl.loop(0, HALF // CHUNK)
        def _(step):
            start = pl.multiple_of(step * CHUNK, CHUNK)
            body(pl.ds(start, CHUNK), pl.multiple_of(half * HALF + start, CHUNK))

    return run


def masks_of(offs, base):
    shape = (CHUNK, PROBE)
    return [
        (outside(shape, 0, base, offs[2 * s]), outside(shape, 1, 0, offs[2 * s + 1]))
        for s in range(SLOTS)
    ]


def gather_windows(offs, wide, row_a, row_b, target):
    for source, half in row_halves(offs, row_a, row_b, True):

        @chunks(half)
        def _(part_rows, base):
            rows = pl.ds(base, CHUNK)
            for slot, (row_out, col_out) in enumerate(masks_of(offs, base)):
                for part in range(2):
                    own = wide[part, rows, :]
                    other = source[part, part_rows, :]
                    near = jnp.where(row_out, other[:, :PROBE], own[:, :PROBE])
                    across = jnp.where(row_out, other[:, PROBE:], own[:, PROBE:])
                    target[slot, part, rows, :] = jnp.where(col_out, across, near)


def spread(offs, contrib, kept, send_a, send_b):
    for target, half in row_halves(offs, send_a, send_b, True):

        @chunks(half)
        def _(part_rows, base):
            rows = pl.ds(base, CHUNK)
            masks = masks_of(offs, base)
            for part in range(2):
                totals = [None] * 4
                for slot, (row_out, col_out) in enumerate(masks):
                    value = contrib[slot, part, rows, :]
                    zero = jnp.zeros_like(value)
                    inner = jnp.where(row_out, zero, value)
                    outer = jnp.where(row_out, value, zero)
                    pieces = [
                        jnp.where(col_out, zero, inner),
                        jnp.where(col_out, inner, zero),
                        jnp.where(col_out, zero, outer),
                        jnp.where(col_out, outer, zero),
                    ]
                    totals = [p if t is None else t + p for t, p in zip(totals, pieces)]
                kept[part, rows, :PROBE] = totals[0]
                kept[part, rows, PROBE:] = totals[1]
                target[part, part_rows, :PROBE] = totals[2]
                target[part, part_rows, PROBE:] = totals[3]


def times(ar, ai, br, bi):
    return ar * br - ai * bi, ar * bi + ai * br


def conj_times(ar, ai, br, bi):
    return ar * br + ai * bi, ar * bi - ai * br


def forward_kernel(offs, wide, row_a, row_b, rolled, tab, wave, window, work):
    gather_windows(offs, wide, row_a, row_b, window)
    for s in range(SLOTS):
        value = times(rolled[s, 0], rolled[s, 1], window[s, 0], window[s, 1])
        work[s, 0], work[s, 1] = pass_along(*value, 1, tab, E, O, True, True)
    for s in range(SLOTS):
        wave[s, 0], wave[s, 1] = pass_along(work[s, 0], work[s, 1], 0, tab, ET, OT, True, True)


def middle_kernel(
    offs, wide, row_a, row_b, wave, ordered, tab, kept, send_a, send_b, back, window, work, held
):
    gather_windows(offs, wide, row_a, row_b, window)
    for s in range(SLOTS):
        value = times(wave[s, 0], wave[s, 1], window[s, 0], window[s, 1])
        held[s, 0], held[s, 1] = pass_along(*value, 1, tab, E, O, True, False)
    for s in range(SLOTS):
        weight = jnp.where(s < offs[2 * SLOTS], 1.0, 0.0).astype(F32)
        fr, fi = pass_along(held[s, 0], held[s, 1], 0, tab, ET, OT, True, False)
        factor = weight * (fr * fr + fi * fi - ordered[s])
        work[s, 0], work[s, 1] = factor * fr, factor * fi
    for s in range(SLOTS):
        held[s, 0], held[s, 1] = pass_along(work[s, 0], work[s, 1], 0, tab, E, O, False, True)
    for s in range(SLOTS):
        value = pass_along(held[s, 0], held[s, 1], 1, tab, ET, OT, False, True)
        work[s, 0], work[s, 1] = conj_times(wave[s, 0], wave[s, 1], *value)
        back[s, 0], back[s, 1] = conj_times(window[s, 0], window[s, 1], *value)
    spread(offs, work, kept, send_a, send_b)


def backward_kernel(offs, back, rolled, tab, kept, send_a, send_b, held, work):
    for s in range(SLOTS):
        held[s, 0], held[s, 1] = pass_along(back[s, 0], back[s, 1], 1, tab, ET, OT, True, True)
    for s in range(SLOTS):
        value = pass_along(held[s, 0], held[s, 1], 0, tab, E, O, True, True)
        work[s, 0], work[s, 1] = conj_times(rolled[s, 0], rolled[s, 1], *value)
    spread(offs, work, kept, send_a, send_b)


def widen_kernel(offs, own, right, left, wide, send_a, send_b):
    for target, half in row_halves(offs, send_a, send_b, False):

        @chunks(half)
        def _(part_rows, base):
            rows = pl.ds(base, CHUNK)
            for part in range(2):
                for ref, here in ((wide, rows), (target, part_rows)):
                    ref[part, here, :256] = own[part, rows, :]
                    ref[part, here, 256:384] = right[part, rows, :]
                    ref[part, here, 384:] = left[part, rows, :]


def fold_middle_kernel(offs, kept, row_a, row_b, total, to_right, to_left):
    for source, half in row_halves(offs, row_a, row_b, False):

        @chunks(half)
        def _(part_rows, base):
            rows = pl.ds(base, CHUNK)
            for part in range(2):
                value = kept[part, rows, :] + source[part, part_rows, :]
                total[part, rows, :] = value
                to_right[part, rows, :HALF] = value[:, 256:384]
                to_right[part, rows, HALF:] = value[:, 128:256]
                to_left[part, rows, :HALF] = value[:, 0:128]
                to_left[part, rows, HALF:] = value[:, 384:512]


def fold_last_kernel(offs, kept, row_a, row_b, total, to_right, to_left):
    for source, half in row_halves(offs, row_a, row_b, False):

        @chunks(half)
        def _(part_rows, base):
            rows = pl.ds(base, CHUNK)
            for part in range(2):
                value = kept[part, rows, :] + source[part, part_rows, :]
                total[part, rows, :] = value[:, :256]
                to_right[part, rows, :] = value[:, 256:384]
                to_left[part, rows, :] = value[:, 384:512]


def update_middle_kernel(offs, wide, total, from_left, from_right, after, send_a, send_b):
    for target, half in row_halves(offs, send_a, send_b, False):

        @chunks(half)
        def _(part_rows, base):
            rows = pl.ds(base, CHUNK)
            for part in range(2):
                low, high = from_left[part, rows, :], from_right[part, rows, :]
                came = jnp.concatenate(
                    [low[:, :HALF], high[:, HALF:], high[:, :HALF], low[:, HALF:]], axis=1
                )
                value = wide[part, rows, :] - STEP_SIZE * (total[part, rows, :] + came)
                after[part, rows, :] = value
                target[part, part_rows, :] = value


def updated(wide, total, from_left, from_right, part, rows):
    came = jnp.concatenate([from_left[part, rows, :], from_right[part, rows, :]], axis=1)
    return wide[part, rows, :PROBE] - STEP_SIZE * (total[part, rows, :] + came)


def update_last_kernel(wide, total, from_left, from_right, after):
    @pl.loop(0, PROBE // CHUNK)
    def _(step):
        rows = pl.ds(pl.multiple_of(step * CHUNK, CHUNK), CHUNK)
        for part in range(2):
            after[part, rows, :] = updated(wide, total, from_left, from_right, part, rows)


def finish_kernel(wide, total, from_left, from_right, other, after):
    @pl.loop(0, PROBE // CHUNK)
    def _(step):
        rows = pl.ds(pl.multiple_of(step * CHUNK, CHUNK), CHUNK)
        for part in range(2):
            after[part, rows, :] = updated(wide, total, from_left, from_right, part, rows)
            after[part + 2, rows, :] = other[part, rows, :]


WIDE = (2, PROBE, 2 * PROBE)
BAND = (2, HALF, 2 * PROBE)
STRIP = (2, PROBE, HALF)
CORE = (2, PROBE, PROBE)
FIELD = (SLOTS, 2, PROBE, PROBE)


def kernel_call(body, outs, kinds, scratch=(), mib=8, flops=10**7):
    return pl.pallas_call(
        body,
        out_shape=[jax.ShapeDtypeStruct(shape, F32) for shape in outs],
        in_specs=[SMEM if kind == "s" else VMEM for kind in kinds],
        out_specs=[VMEM] * len(outs),
        scratch_shapes=list(scratch),
        compiler_params=pltpu.CompilerParams(vmem_limit_bytes=mib * 1024 * 1024),
        cost_estimate=pl.CostEstimate(flops=flops, bytes_accessed=10**6, transcendentals=0),
    )


def shifted(value, axis, steps):
    count = lax.axis_size(axis)
    return lax.ppermute(value, axis, [(i, (i + steps) % count) for i in range(count)])


def swapped(value, axis, odd):
    count = lax.axis_size(axis)
    pairs = []
    for low in range(odd, count + odd, 2):
        one, two = low % count, (low + 1) % count
        pairs += [(one, two), (two, one)]
    return lax.ppermute(value, axis, pairs)


def swap_rows(send_a, send_b):
    row_b = swapped(send_b, "row", 1)
    return swapped(send_a, "row", 0), row_b


def local(object_core, probe_field, offsets, tile_counts, intensity):
    parity = lax.axis_index("row") % 2
    scalars = jnp.concatenate(
        [offsets.reshape(-1), tile_counts.reshape(-1), parity.astype(jnp.int32).reshape(1)]
    )
    fourier, space = (jnp.asarray(t) for t in tables())
    field = pltpu.VMEM(FIELD, F32)

    own = [object_core[2 * k : 2 * k + 2] for k in range(SLICES)]
    beside = []
    for cells in own:
        right = shifted(cells[:, :, :HALF], "col", -1)
        left = shifted(cells[:, :, HALF:], "col", 1)
        beside.append((right, left))
    rolled, ordered = kernel_call(
        prepare_kernel,
        [FIELD, (SLOTS, PROBE, PROBE)],
        "svv",
        [pltpu.VMEM((2, PROBE, PROBE), BF16)],
        16,
        3 * 10**9,
    )(scalars, probe_field, intensity[0, 0])
    wide, rows = [None] * SLICES, [None] * SLICES
    for k in range(SLICES):
        wide[k], send_a, send_b = kernel_call(widen_kernel, [WIDE, BAND, BAND], "svvv")(
            scalars, own[k], *beside[k]
        )
        rows[k] = swap_rows(send_a, send_b)
    for iteration in range(ITERS):
        last = iteration == ITERS - 1
        (wave,) = kernel_call(
            forward_kernel, [FIELD], "svvvvv", [field] * 2, 20, 3 * 10**9
        )(scalars, wide[0], *rows[0], rolled, space)
        kept1, send_a, send_b, back = kernel_call(
            middle_kernel, [WIDE, BAND, BAND, FIELD], "svvvvvv", [field] * 3, 24, 6 * 10**9
        )(scalars, wide[1], *rows[1], wave, ordered, fourier)
        rows1 = swap_rows(send_a, send_b)
        kept0, send_a, send_b = kernel_call(
            backward_kernel, [WIDE, BAND, BAND], "svvv", [field] * 2, 20, 4 * 10**9
        )(scalars, back, rolled, space)
        rows0 = swap_rows(send_a, send_b)
        kept, back_rows = [kept0, kept1], [rows0, rows1]
        shapes = [CORE, STRIP, STRIP] if last else [WIDE, CORE, CORE]
        fold = fold_last_kernel if last else fold_middle_kernel
        came = [None] * SLICES
        for k in (1, 0):
            total, to_right, to_left = kernel_call(fold, shapes, "svvv")(
                scalars, kept[k], *back_rows[k]
            )
            came[k] = (total, shifted(to_right, "col", 1), shifted(to_left, "col", -1))
        if last:
            (other,) = kernel_call(update_last_kernel, [CORE], "vvvv")(wide[1], *came[1])
            (after,) = kernel_call(finish_kernel, [(CHANNELS, PROBE, PROBE)], "vvvvv")(
                wide[0], *came[0], other
            )
            return after
        for k in (1, 0):
            wide[k], send_a, send_b = kernel_call(
                update_middle_kernel, [WIDE, BAND, BAND], "svvvv"
            )(scalars, wide[k], *came[k])
            rows[k] = swap_rows(send_a, send_b)


def solution(mesh):
    placed = (
        P(None, "row", "col"),
        P(),
        P("row", "col", None, None),
        P("row", "col"),
        P("row", "col", None, None, None),
    )
    return jax.shard_map(
        local, mesh=mesh, in_specs=placed, out_specs=P(None, "row", "col"), check_vma=False
    )
```

```python
import functools

import jax
import jax.numpy as jnp
import numpy as np
from jax import lax
from jax.experimental import pallas as pl
from jax.experimental.pallas import tpu as pltpu
from jax.sharding import PartitionSpec as P


PROBE = 256
HALF = 128
SLICES = 2
SLOTS = 3
ITERS = 2
CHANNELS = 2 * SLICES
FRESNEL = 24.0
STEP_SIZE = 0.05
CHUNK = 32

F32 = jnp.float32
BF16 = jnp.bfloat16
VMEM = pl.BlockSpec(memory_space=pltpu.VMEM)
SMEM = pl.BlockSpec(memory_space=pltpu.SMEM)

E, O, ET, OT = range(4)


def real_form(matrix):
    return np.block([[matrix.real, matrix.imag], [-matrix.imag, matrix.real]])


def stack_of(one, two):
    forms = [real_form(one), real_form(two)]
    forms = np.stack(forms + [m.T for m in forms]).astype(np.float32)
    high = forms.astype(BF16)
    low = (forms - high.astype(np.float32)).astype(BF16)
    return np.concatenate([high, low])


def tables():
    n = np.arange(HALF)
    even = np.exp(-2j * np.pi * ((2 * np.outer(n, n)) % PROBE) / PROBE) / math_root()
    odd = np.exp(-2j * np.pi * ((n[:, None] * (2 * n[None, :] + 1)) % PROBE) / PROBE) / math_root()
    whole = np.arange(PROBE)
    frequency = ((whole + HALF) % PROBE - HALF) / PROBE
    response = np.exp(-1j * np.pi * FRESNEL * frequency**2)
    first = np.fft.ifft(response)
    circulant = first[(whole[:, None] - whole[None, :]) % PROBE]
    near, far = circulant[:HALF, :HALF], circulant[:HALF, HALF:]
    return stack_of(even, odd), stack_of((near + far) / 2, (near - far) / 2)


def math_root():
    return float(np.sqrt(PROBE))


def dot(left, right):
    return jnp.dot(left, right, preferred_element_type=F32)


def parts(values):
    high = values.astype(BF16)
    low = (values - high.astype(F32)).astype(BF16)
    return high, low


def right_dot(values, tab, number):
    high, low = parts(values)
    return dot(high, tab[number]) + (dot(low, tab[number]) + dot(high, tab[number + 4]))


def left_dot(tab, number, values):
    high, low = parts(values)
    return dot(tab[number], high) + (dot(tab[number + 4], high) + dot(tab[number], low))


def halves(values, axis):
    if axis == 1:
        return values[:, :HALF], values[:, HALF:]
    return values[:HALF, :], values[HALF:, :]


def pass_along(real, imag, axis, tab, first, second, before, after):
    r0, r1 = halves(real, axis)
    i0, i1 = halves(imag, axis)
    if before:
        r0, r1, i0, i1 = r0 + r1, r0 - r1, i0 + i1, i0 - i1
    u = jnp.concatenate([r0, i0], axis=axis)
    v = jnp.concatenate([r1, i1], axis=axis)
    if axis == 1:
        u, v = right_dot(u, tab, first), right_dot(v, tab, second)
    else:
        u, v = left_dot(tab, first, u), left_dot(tab, second, v)
    r0, i0 = halves(u, axis)
    r1, i1 = halves(v, axis)
    if after:
        r0, r1, i0, i1 = r0 + r1, r0 - r1, i0 + i1, i0 - i1
    return jnp.concatenate([r0, r1], axis=axis), jnp.concatenate([i0, i1], axis=axis)


def outside(shape, axis, base, offset):
    place = lax.broadcasted_iota(jnp.int32, shape, axis) + base
    start = offset - HALF
    return (place < start) | (place >= start + PROBE)


def ordering():
    row = lax.broadcasted_iota(jnp.int32, (PROBE, PROBE), 0)
    column = lax.broadcasted_iota(jnp.int32, (PROBE, PROBE), 1)
    wanted = jnp.where(column < HALF, 2 * column, 2 * column - (PROBE - 1))
    back = jnp.where(row < HALF, 2 * row, 2 * row - (PROBE - 1))
    one = jnp.where(row == wanted, 1.0, 0.0).astype(BF16)
    two = jnp.where(column == back, 1.0, 0.0).astype(BF16)
    return one, two


def prepare_kernel(offs, probe, intensity, rolled, ordered, order):
    order[0], order[1] = ordering()
    for slot in range(SLOTS):
        for part in range(2):
            value = pltpu.roll(probe[part], (offs[2 * slot] + HALF) & (PROBE - 1), 0)
            rolled[slot, part] = pltpu.roll(value, (offs[2 * slot + 1] + HALF) & (PROBE - 1), 1)

    @pl.loop(0, SLOTS)
    def _(slot):
        for axis in (1, 0):
            value = ordered[slot] if axis == 0 else intensity[slot]
            high = value.astype(BF16)
            rest = value - high.astype(F32)
            middle = rest.astype(BF16)
            low = (rest - middle.astype(F32)).astype(BF16)
            if axis == 1:
                value = (dot(high, order[0]) + dot(middle, order[0])) + dot(low, order[0])
            else:
                value = (dot(order[1], high) + dot(order[1], middle)) + dot(order[1], low)
            ordered[slot] = value


def row_halves(offs, one, two, first):
    parity = offs[2 * SLOTS + 1]
    return ((one, parity), (two, 1 - parity)) if first else ((one, 1 - parity), (two, parity))


def chunks(half):
    def run(body):
        @pl.loop(0, HALF // CHUNK)
        def _(step):
            start = pl.multiple_of(step * CHUNK, CHUNK)
            body(pl.ds(start, CHUNK), pl.multiple_of(half * HALF + start, CHUNK))

    return run


def masks_of(offs, base):
    shape = (CHUNK, PROBE)
    return [
        (outside(shape, 0, base, offs[2 * s]), outside(shape, 1, 0, offs[2 * s + 1]))
        for s in range(SLOTS)
    ]


def gather_windows(offs, wide, row_a, row_b, target):
    for source, half in row_halves(offs, row_a, row_b, True):

        @chunks(half)
        def _(part_rows, base):
            rows = pl.ds(base, CHUNK)
            for slot, (row_out, col_out) in enumerate(masks_of(offs, base)):
                for part in range(2):
                    own = wide[part, rows, :]
                    other = source[part, part_rows, :]
                    near = jnp.where(row_out, other[:, :PROBE], own[:, :PROBE])
                    across = jnp.where(row_out, other[:, PROBE:], own[:, PROBE:])
                    target[slot, part, rows, :] = jnp.where(col_out, across, near)


def spread(offs, contrib, kept, send_a, send_b):
    for target, half in row_halves(offs, send_a, send_b, True):

        @chunks(half)
        def _(part_rows, base):
            rows = pl.ds(base, CHUNK)
            masks = masks_of(offs, base)
            for part in range(2):
                totals = [None] * 4
                for slot, (row_out, col_out) in enumerate(masks):
                    value = contrib[slot, part, rows, :]
                    zero = jnp.zeros_like(value)
                    inner = jnp.where(row_out, zero, value)
                    outer = jnp.where(row_out, value, zero)
                    pieces = [
                        jnp.where(col_out, zero, inner),
                        jnp.where(col_out, inner, zero),
                        jnp.where(col_out, zero, outer),
                        jnp.where(col_out, outer, zero),
                    ]
                    totals = [p if t is None else t + p for t, p in zip(totals, pieces)]
                kept[part, rows, :PROBE] = totals[0]
                kept[part, rows, PROBE:] = totals[1]
                target[part, part_rows, :PROBE] = totals[2]
                target[part, part_rows, PROBE:] = totals[3]


def times(ar, ai, br, bi):
    return ar * br - ai * bi, ar * bi + ai * br


def conj_times(ar, ai, br, bi):
    return ar * br + ai * bi, ar * bi - ai * br


def forward_kernel(offs, wide, row_a, row_b, rolled, tab, wave, window, work):
    gather_windows(offs, wide, row_a, row_b, window)
    for s in range(SLOTS):
        value = times(rolled[s, 0], rolled[s, 1], window[s, 0], window[s, 1])
        work[s, 0], work[s, 1] = pass_along(*value, 1, tab, E, O, True, True)
    for s in range(SLOTS):
        wave[s, 0], wave[s, 1] = pass_along(work[s, 0], work[s, 1], 0, tab, ET, OT, True, True)


def middle_kernel(
    offs, wide, row_a, row_b, wave, ordered, tab, kept, send_a, send_b, back, window, work, held
):
    gather_windows(offs, wide, row_a, row_b, window)
    for s in range(SLOTS):
        value = times(wave[s, 0], wave[s, 1], window[s, 0], window[s, 1])
        held[s, 0], held[s, 1] = pass_along(*value, 1, tab, E, O, True, False)
    for s in range(SLOTS):
        weight = jnp.where(s < offs[2 * SLOTS], 1.0, 0.0).astype(F32)
        fr, fi = pass_along(held[s, 0], held[s, 1], 0, tab, ET, OT, True, False)
        factor = weight * (fr * fr + fi * fi - ordered[s])
        work[s, 0], work[s, 1] = factor * fr, factor * fi
    for s in range(SLOTS):
        held[s, 0], held[s, 1] = pass_along(work[s, 0], work[s, 1], 0, tab, E, O, False, True)
    for s in range(SLOTS):
        value = pass_along(held[s, 0], held[s, 1], 1, tab, ET, OT, False, True)
        work[s, 0], work[s, 1] = conj_times(wave[s, 0], wave[s, 1], *value)
        back[s, 0], back[s, 1] = conj_times(window[s, 0], window[s, 1], *value)
    spread(offs, work, kept, send_a, send_b)


def backward_kernel(offs, back, rolled, tab, kept, send_a, send_b, held, work):
    for s in range(SLOTS):
        held[s, 0], held[s, 1] = pass_along(back[s, 0], back[s, 1], 1, tab, ET, OT, True, True)
    for s in range(SLOTS):
        value = pass_along(held[s, 0], held[s, 1], 0, tab, E, O, True, True)
        work[s, 0], work[s, 1] = conj_times(rolled[s, 0], rolled[s, 1], *value)
    spread(offs, work, kept, send_a, send_b)


def widen_kernel(first, offs, own, right, left, wide, send_a, send_b):
    for target, half in row_halves(offs, send_a, send_b, False):

        @chunks(half)
        def _(part_rows, base):
            rows = pl.ds(base, CHUNK)
            for part in range(2):
                for ref, here in ((wide, rows), (target, part_rows)):
                    ref[part, here, :256] = own[first + part, rows, :]
                    ref[part, here, 256:384] = right[part, rows, :]
                    ref[part, here, 384:] = left[part, rows, :]


def fold_middle_kernel(offs, kept, row_a, row_b, total, to_right, to_left):
    for source, half in row_halves(offs, row_a, row_b, False):

        @chunks(half)
        def _(part_rows, base):
            rows = pl.ds(base, CHUNK)
            for part in range(2):
                value = kept[part, rows, :] + source[part, part_rows, :]
                total[part, rows, :] = value
                to_right[part, rows, :HALF] = value[:, 256:384]
                to_right[part, rows, HALF:] = value[:, 128:256]
                to_left[part, rows, :HALF] = value[:, 0:128]
                to_left[part, rows, HALF:] = value[:, 384:512]


def fold_last_kernel(offs, kept, row_a, row_b, total, to_right, to_left):
    for source, half in row_halves(offs, row_a, row_b, False):

        @chunks(half)
        def _(part_rows, base):
            rows = pl.ds(base, CHUNK)
            for part in range(2):
                value = kept[part, rows, :] + source[part, part_rows, :]
                total[part, rows, :] = value[:, :256]
                to_right[part, rows, :] = value[:, 256:384]
                to_left[part, rows, :] = value[:, 384:512]


def update_middle_kernel(offs, wide, total, from_left, from_right, after, send_a, send_b):
    for target, half in row_halves(offs, send_a, send_b, False):

        @chunks(half)
        def _(part_rows, base):
            rows = pl.ds(base, CHUNK)
            for part in range(2):
                low, high = from_left[part, rows, :], from_right[part, rows, :]
                came = jnp.concatenate(
                    [low[:, :HALF], high[:, HALF:], high[:, :HALF], low[:, HALF:]], axis=1
                )
                value = wide[part, rows, :] - STEP_SIZE * (total[part, rows, :] + came)
                after[part, rows, :] = value
                target[part, part_rows, :] = value


def updated(wide, total, from_left, from_right, part, rows):
    came = jnp.concatenate([from_left[part, rows, :], from_right[part, rows, :]], axis=1)
    return wide[part, rows, :PROBE] - STEP_SIZE * (total[part, rows, :] + came)


def update_last_kernel(wide, total, from_left, from_right, after):
    @pl.loop(0, PROBE // CHUNK)
    def _(step):
        rows = pl.ds(pl.multiple_of(step * CHUNK, CHUNK), CHUNK)
        for part in range(2):
            after[part, rows, :] = updated(wide, total, from_left, from_right, part, rows)


def finish_kernel(wide, total, from_left, from_right, other, after):
    @pl.loop(0, PROBE // CHUNK)
    def _(step):
        rows = pl.ds(pl.multiple_of(step * CHUNK, CHUNK), CHUNK)
        for part in range(2):
            after[part, rows, :] = updated(wide, total, from_left, from_right, part, rows)
            after[part + 2, rows, :] = other[part, rows, :]


WIDE = (2, PROBE, 2 * PROBE)
BAND = (2, HALF, 2 * PROBE)
STRIP = (2, PROBE, HALF)
CORE = (2, PROBE, PROBE)
FIELD = (SLOTS, 2, PROBE, PROBE)


def kernel_call(body, outs, kinds, scratch=(), mib=8, flops=10**7):
    return pl.pallas_call(
        body,
        out_shape=[jax.ShapeDtypeStruct(shape, F32) for shape in outs],
        in_specs=[SMEM if kind == "s" else VMEM for kind in kinds],
        out_specs=[VMEM] * len(outs),
        scratch_shapes=list(scratch),
        compiler_params=pltpu.CompilerParams(vmem_limit_bytes=mib * 1024 * 1024),
        cost_estimate=pl.CostEstimate(flops=flops, bytes_accessed=10**6, transcendentals=0),
    )


def shifted(value, axis, steps):
    count = lax.axis_size(axis)
    return lax.ppermute(value, axis, [(i, (i + steps) % count) for i in range(count)])


def swapped(value, axis, odd):
    count = lax.axis_size(axis)
    pairs = []
    for low in range(odd, count + odd, 2):
        one, two = low % count, (low + 1) % count
        pairs += [(one, two), (two, one)]
    return lax.ppermute(value, axis, pairs)


def swap_rows(send_a, send_b):
    row_b = swapped(send_b, "row", 1)
    return swapped(send_a, "row", 0), row_b


def pass_cols(to_right, to_left):
    return shifted(to_right, "col", 1), shifted(to_left, "col", -1)


def local(object_core, probe_field, offsets, tile_counts, intensity):
    parity = lax.axis_index("row") % 2
    scalars = jnp.concatenate(
        [offsets.reshape(-1), tile_counts.reshape(-1), parity.astype(jnp.int32).reshape(1)]
    )
    fourier, space = (jnp.asarray(t) for t in tables())
    field = pltpu.VMEM(FIELD, F32)

    own = [object_core[2 * k : 2 * k + 2] for k in range(SLICES)]
    beside = [pass_cols(cells[:, :, HALF:], cells[:, :, :HALF]) for cells in own]
    rolled, ordered = kernel_call(
        prepare_kernel,
        [FIELD, (SLOTS, PROBE, PROBE)],
        "svv",
        [pltpu.VMEM((2, PROBE, PROBE), BF16)],
        16,
        3 * 10**9,
    )(scalars, probe_field, intensity[0, 0])
    wide, rows = [None] * SLICES, [None] * SLICES
    for k in range(SLICES):
        left, right = beside[k]
        wide[k], send_a, send_b = kernel_call(
            functools.partial(widen_kernel, 2 * k), [WIDE, BAND, BAND], "svvv"
        )(scalars, object_core, right, left)
        rows[k] = swap_rows(send_a, send_b)
    for iteration in range(ITERS):
        last = iteration == ITERS - 1
        (wave,) = kernel_call(
            forward_kernel, [FIELD], "svvvvv", [field] * 2, 20, 3 * 10**9
        )(scalars, wide[0], *rows[0], rolled, space)
        kept1, send_a, send_b, back = kernel_call(
            middle_kernel, [WIDE, BAND, BAND, FIELD], "svvvvvv", [field] * 3, 24, 6 * 10**9
        )(scalars, wide[1], *rows[1], wave, ordered, fourier)
        rows1 = swap_rows(send_a, send_b)
        kept0, send_a, send_b = kernel_call(
            backward_kernel, [WIDE, BAND, BAND], "svvv", [field] * 2, 20, 4 * 10**9
        )(scalars, back, rolled, space)
        rows0 = swap_rows(send_a, send_b)
        kept, back_rows = [kept0, kept1], [rows0, rows1]
        shapes = [CORE, STRIP, STRIP] if last else [WIDE, CORE, CORE]
        fold = fold_last_kernel if last else fold_middle_kernel
        came = [None] * SLICES
        for k in (1, 0):
            total, to_right, to_left = kernel_call(fold, shapes, "svvv")(
                scalars, kept[k], *back_rows[k]
            )
            came[k] = (total, *pass_cols(to_right, to_left))
        if last:
            (other,) = kernel_call(update_last_kernel, [CORE], "vvvv")(wide[1], *came[1])
            (after,) = kernel_call(finish_kernel, [(CHANNELS, PROBE, PROBE)], "vvvvv")(
                wide[0], *came[0], other
            )
            return after
        for k in (1, 0):
            wide[k], send_a, send_b = kernel_call(
                update_middle_kernel, [WIDE, BAND, BAND], "svvvv"
            )(scalars, wide[k], *came[k])
            rows[k] = swap_rows(send_a, send_b)


def solution(mesh):
    placed = (
        P(None, "row", "col"),
        P(),
        P("row", "col", None, None),
        P("row", "col"),
        P("row", "col", None, None, None),
    )
    return jax.shard_map(
        local, mesh=mesh, in_specs=placed, out_specs=P(None, "row", "col"), check_vma=False
    )
```
